32 devices in a mesh: dp: 4 (over y, z), sp: 8 (over x, core).
Axes of the slice: x: 4, y: 2, z: 2, core: 2. Of those that a mesh axis runs over, the one named last changes fastest.
The devices are a block of a 4x4x8 slice.
Arguments:
- tokens: bfloat16 [24, 4096, 2560], P('dp', 'sp'), parts along dimension 0
- w_query: bfloat16 [2560, 4096], replicated
- w_key: bfloat16 [2560, 1024], replicated
- w_value: bfloat16 [2560, 1024], replicated
- w_out: bfloat16 [4096, 2560], replicated
- attn_norm: bfloat16 [2560], replicated
- q_norm: bfloat16 [128], replicated
- k_norm: bfloat16 [128], replicated
Outputs:
- output 1: bfloat16 [24, 4096, 2560], P('dp', 'sp'), parts along dimension 0
- output 2: bfloat16 [24, 4096, 8, 128], P('dp', 'sp'), parts along dimension 0
- output 3: bfloat16 [24, 4096, 8, 128], P('dp', 'sp'), parts along dimension 0
There are 4 independent parts. The reference program is written for one: setup_inputs(seed, part) draws one part's arguments, and reference() takes and returns one part's arrays. A program takes and returns all parts, laid end to end along the dimension named above; an argument that names none is the same for every part.
All inputs are finite; a program needn't handle non-finite values.
Results may differ from the reference program's by a relative error of at most 0.00828171.
Values are sent between devices in bfloat16 or wider.
A program may use at most 768 MiB of HBM per device.

```python
import jax
import jax.numpy as jnp
from jax import lax

BATCH = 6
SEQ_LEN = 4096
D_MODEL = 2560
HEADS = 32
KV_HEADS = 8
HEAD_DIM = 128
EPS = 1e-6
THETA = 1000000.0
Q_BLOCK = min(128, SEQ_LEN)
N_QBLK = SEQ_LEN // Q_BLOCK
GROUP = HEADS // KV_HEADS
SCALE = HEAD_DIM ** -0.5


def rms_norm(values, gain_vec):
    wide_vals = values.astype(jnp.float32)
    inv_rms = lax.rsqrt(jnp.mean(wide_vals * wide_vals, axis=-1, keepdims=True) + EPS)
    return wide_vals * inv_rms * gain_vec.astype(jnp.float32)


def rope_rotate(values, positions):
    half_dim = HEAD_DIM // 2
    inv_freq = THETA ** (-jnp.arange(half_dim, dtype=jnp.float32) * 2.0 / HEAD_DIM)
    angles = positions.astype(jnp.float32)[:, None] * inv_freq[None, :]
    cos_t = jnp.cos(angles)[None, :, None, :]
    sin_t = jnp.sin(angles)[None, :, None, :]
    lo_half = values[..., :half_dim]
    hi_half = values[..., half_dim:]
    return jnp.concatenate([lo_half * cos_t - hi_half * sin_t, hi_half * cos_t + lo_half * sin_t], axis=-1)


def setup_inputs(seed: int = 0, part: int = 0) -> dict:
    part_key = jax.random.fold_in(jax.random.key(seed), part)
    noise_key, walk_key = jax.random.split(part_key, 2)
    shared = jax.random.split(jax.random.key(seed + 1), 7)
    noise_part = 0.5 * jax.random.normal(noise_key, (BATCH, SEQ_LEN, D_MODEL), jnp.float32)
    walk_steps = jax.random.normal(walk_key, (BATCH, SEQ_LEN, D_MODEL), jnp.float32)
    walk_part = jnp.cumsum(walk_steps, axis=1) * (1.5 / SEQ_LEN ** 0.5)
    tokens = (noise_part + walk_part).astype(jnp.bfloat16)

    def make_dense(rng_key, fan_in, fan_out):
        return (jax.random.normal(rng_key, (fan_in, fan_out), jnp.float32) * fan_in ** -0.5).astype(jnp.bfloat16)

    def draw_gain(rng_key, n_elems, center, spread):
        return (center + spread * jax.random.normal(rng_key, (n_elems,), jnp.float32)).astype(jnp.bfloat16)

    return {
        'tokens': tokens,
        'w_query': make_dense(shared[0], D_MODEL, HEADS * HEAD_DIM),
        'w_key': make_dense(shared[1], D_MODEL, KV_HEADS * HEAD_DIM),
        'w_value': make_dense(shared[2], D_MODEL, KV_HEADS * HEAD_DIM),
        'w_out': make_dense(shared[3], HEADS * HEAD_DIM, D_MODEL),
        'attn_norm': draw_gain(shared[4], D_MODEL, 1.0, 0.3),
        'q_norm': draw_gain(shared[5], HEAD_DIM, 1.4, 0.4),
        'k_norm': draw_gain(shared[6], HEAD_DIM, 1.4, 0.4),
    }


def reference(tokens, w_query, w_key, w_value, w_out, attn_norm, q_norm, k_norm):
    hidden = rms_norm(tokens, attn_norm).astype(jnp.bfloat16).reshape(BATCH * SEQ_LEN, D_MODEL)
    q_proj = jnp.dot(hidden, w_query, preferred_element_type=jnp.float32).astype(jnp.bfloat16).reshape(BATCH, SEQ_LEN, HEADS, HEAD_DIM)
    k_proj = jnp.dot(hidden, w_key, preferred_element_type=jnp.float32).astype(jnp.bfloat16).reshape(BATCH, SEQ_LEN, KV_HEADS, HEAD_DIM)
    v_proj = jnp.dot(hidden, w_value, preferred_element_type=jnp.float32).astype(jnp.bfloat16).reshape(BATCH, SEQ_LEN, KV_HEADS, HEAD_DIM)
    positions = jnp.arange(SEQ_LEN)
    q_rot = rope_rotate(rms_norm(q_proj, q_norm), positions).astype(jnp.bfloat16)
    k_rot = rope_rotate(rms_norm(k_proj, k_norm), positions).astype(jnp.bfloat16)
    key_pos = jnp.arange(SEQ_LEN)
    row_ids = jnp.arange(Q_BLOCK)

    def one_seq(seq_args):
        q_seq, k_seq, v_seq = seq_args
        k_wide = k_seq.astype(jnp.float32)
        v_wide = v_seq.astype(jnp.float32)
        q_blocks = q_seq.reshape(N_QBLK, Q_BLOCK, KV_HEADS, GROUP, HEAD_DIM)

        def one_block(blk_args):
            q_blk, blk_idx = blk_args
            scores = jnp.einsum('qkgd,skd->kgqs', q_blk.astype(jnp.float32), k_wide) * SCALE
            allowed = key_pos[None, :] <= (blk_idx * Q_BLOCK + row_ids)[:, None]
            scores = jnp.where(allowed[None, None], scores, -jnp.inf)
            probs_blk = jax.nn.softmax(scores, axis=-1)
            return jnp.einsum('kgqs,skd->qkgd', probs_blk, v_wide).astype(jnp.bfloat16)

        attn_blocks = lax.map(one_block, (q_blocks, jnp.arange(N_QBLK)))
        return attn_blocks.reshape(SEQ_LEN, HEADS * HEAD_DIM)

    attn_out = lax.map(one_seq, (q_rot, k_rot, v_proj))
    proj_out = jnp.dot(attn_out.reshape(BATCH * SEQ_LEN, HEADS * HEAD_DIM), w_out, preferred_element_type=jnp.float32)
    output = (tokens.astype(jnp.float32) + proj_out.reshape(BATCH, SEQ_LEN, D_MODEL)).astype(jnp.bfloat16)
    return (output, k_rot, v_proj)
```

```python
import functools
import math

import jax
import jax.numpy as jnp
from jax import lax
from jax.experimental import pallas as pl
from jax.experimental.pallas import tpu as pltpu
from jax.sharding import PartitionSpec as P


EPS = 1e-6
THETA = 1000000.0
HEAD_DIM = 128
N_SPLIT = 3
ORDER = [
    ('qkv', 0), ('qkv', 1), ('qkv', 2), ('att', 0), ('qkv', 3), ('att', 1), ('qkv', 4), ('att', 2), ('qkv', 5),
    ('att', 3), ('out', 0), ('out', 1), ('out', 2), ('out', 3), ('att', 4), ('out', 4), ('att', 5), ('out', 5),
]
VMEM_LIMIT = 60 * 1024 * 1024


def rope_tables(positions):
    half_dim = HEAD_DIM // 2
    inv_freq = THETA ** (-jnp.arange(half_dim, dtype=jnp.float32) * 2.0 / HEAD_DIM)
    angles = positions.astype(jnp.float32)[:, None] * inv_freq[None, :]
    cos_t, sin_t = jnp.cos(angles), jnp.sin(angles)
    return jnp.concatenate([cos_t, cos_t], axis=-1), jnp.concatenate([-sin_t, sin_t], axis=-1)


def head_norm_rope(head, gain, cos_t, sin_t):
    wide = head.astype(jnp.float32)
    inv_rms = lax.rsqrt(jnp.mean(wide * wide, axis=-1, keepdims=True) + EPS)
    normed = wide * inv_rms * gain
    return (normed * cos_t + pltpu.roll(normed, HEAD_DIM // 2, 1) * sin_t).astype(jnp.bfloat16)


def qkv_kernel(x_ref, wq_ref, wk_ref, wv_ref, an_ref, qn_ref, kn_ref, cos_ref, sin_ref, *refs):
    send_ref, kc_ref, vc_ref, hid_ref = refs[-4:]
    n_dest, n_slot = send_ref.shape[:2]
    n_group = n_slot - 2
    two = 2 * HEAD_DIM

    @pl.when(pl.program_id(0) == 0)
    def _():
        wide = x_ref[0].astype(jnp.float32)
        inv_rms = lax.rsqrt(jnp.mean(wide * wide, axis=-1, keepdims=True) + EPS)
        hid_ref[...] = (wide * inv_rms * an_ref[...].astype(jnp.float32)).astype(jnp.bfloat16)

    q_gain = qn_ref[...].astype(jnp.float32)
    k_gain = kn_ref[...].astype(jnp.float32)

    def project(weight):
        return jnp.dot(hid_ref[...], weight, preferred_element_type=jnp.float32).astype(jnp.bfloat16)

    def weight_of(job):
        dest, pair = job
        if pair == n_group // 2:
            col = slice(dest * HEAD_DIM, (dest + 1) * HEAD_DIM)
            return jnp.concatenate([wk_ref[:, col], wv_ref[:, col]], axis=1)
        first = dest * n_group * HEAD_DIM + pair * two
        return wq_ref[:, first:first + two]

    def finish(job, both):
        dest, pair = job
        if pair == n_group // 2:
            col = slice(dest * HEAD_DIM, (dest + 1) * HEAD_DIM)
            key = head_norm_rope(both[:, :HEAD_DIM], k_gain, cos_ref[...], sin_ref[...])
            send_ref[dest, n_group] = key
            kc_ref[0, :, col] = key
            send_ref[dest, n_group + 1] = both[:, HEAD_DIM:]
            vc_ref[0, :, col] = both[:, HEAD_DIM:]
            return
        for sub in range(2):
            head = both[:, sub * HEAD_DIM:(sub + 1) * HEAD_DIM]
            send_ref[dest, 2 * pair + sub] = head_norm_rope(head, q_gain, cos_ref[...], sin_ref[...])

    jobs = [(dest, pair) for dest in range(n_dest) for pair in range(n_group // 2 + 1)]
    pending = None
    for job in jobs:
        both = project(weight_of(job))
        if pending is not None:
            finish(*pending)
        pending = (job, both)
    finish(*pending)


def qkv_project(prompt, tokens, w_query, w_key, w_value, attn_norm, q_norm, k_norm, cos_t, sin_t, caches):
    n_batch, n_tok, d_model = tokens.shape
    n_kv = w_key.shape[1] // HEAD_DIM
    n_group = w_query.shape[1] // w_key.shape[1]
    per = 2
    cols = per * HEAD_DIM

    def whole(shape):
        return pl.BlockSpec(shape, lambda s: (0,) * len(shape))

    in_specs = [
        pl.BlockSpec((1, n_tok, d_model), lambda s: (prompt, 0, 0)),
        pl.BlockSpec((d_model, n_group * cols), lambda s: (0, s)),
        pl.BlockSpec((d_model, cols), lambda s: (0, s)),
        pl.BlockSpec((d_model, cols), lambda s: (0, s)),
        whole((1, d_model)), whole((1, HEAD_DIM)), whole((1, HEAD_DIM)),
        whole((n_tok, HEAD_DIM)), whole((n_tok, HEAD_DIM)),
    ]
    args = [tokens, w_query, w_key, w_value, attn_norm, q_norm, k_norm, cos_t, sin_t]
    aliases = {}
    if caches is not None:
        aliases = {len(args): 1, len(args) + 1: 2}
        args += list(caches)
        in_specs += [pl.BlockSpec(memory_space=pl.ANY)] * 2
    flops = 2 * n_tok * d_model * (w_query.shape[1] + 2 * w_key.shape[1])
    return pl.pallas_call(
        qkv_kernel,
        grid=(n_kv // per,),
        in_specs=in_specs,
        out_specs=[
            pl.BlockSpec((per, n_group + 2, n_tok, HEAD_DIM), lambda s: (s, 0, 0, 0)),
            pl.BlockSpec((1, n_tok, cols), lambda s: (prompt, 0, s)),
            pl.BlockSpec((1, n_tok, cols), lambda s: (prompt, 0, s)),
        ],
        out_shape=[
            jax.ShapeDtypeStruct((n_kv, n_group + 2, n_tok, HEAD_DIM), jnp.bfloat16),
            jax.ShapeDtypeStruct((n_batch, n_tok, n_kv * HEAD_DIM), jnp.bfloat16),
            jax.ShapeDtypeStruct((n_batch, n_tok, n_kv * HEAD_DIM), jnp.bfloat16),
        ],
        scratch_shapes=[pltpu.VMEM((n_tok, d_model), jnp.bfloat16)],
        input_output_aliases=aliases,
        compiler_params=pltpu.CompilerParams(vmem_limit_bytes=VMEM_LIMIT),
        cost_estimate=pl.CostEstimate(flops=flops, bytes_accessed=48 << 20, transcendentals=0),
        name="qkv",
    )(*args)


def attention_kernel(gathered, n_full_ref, q_ref, kv_ref, o_ref, qt_ref, vt_ref, m_ref, l_ref, acc_ref):
    n_group, n_tok = q_ref.shape[1], q_ref.shape[2]
    n_full = n_full_ref[0] if gathered else pl.program_id(0)
    scale = HEAD_DIM ** -0.5 * math.log2(math.e)
    lanes = 8

    def keys_of(idx):
        return kv_ref[idx, 0, 0] if gathered else kv_ref[idx, 0]

    def turn_values(idx):
        vt_ref[idx] = (kv_ref[idx, 0, 1] if gathered else kv_ref[idx, 1]).T

    if gathered:
        def turn(j, carry):
            turn_values(j)
            return carry

        lax.fori_loop(0, n_full + 1, turn, 0)
    else:
        turn_values(n_full)
    for g in range(n_group):
        qt_ref[g] = q_ref[0, g].T

    def scores_t(keys, g):
        return jnp.dot(keys, qt_ref[g], preferred_element_type=jnp.float32)

    def weighted_t(idx, probs):
        return jnp.dot(vt_ref[idx], probs.astype(jnp.bfloat16), preferred_element_type=jnp.float32)

    def partial_sum(p):
        return jnp.sum(p.reshape(n_tok // lanes, lanes, n_tok), axis=0)

    def diagonal():
        keys = keys_of(n_full)
        visible = lax.broadcasted_iota(jnp.int32, (n_tok, n_tok), 0) <= lax.broadcasted_iota(jnp.int32, (n_tok, n_tok), 1)
        for g in range(n_group):
            s = jnp.where(visible, scores_t(keys, g) * scale, -jnp.inf)
            top = jnp.max(s, axis=0, keepdims=True)
            p = jnp.exp2(s - top)
            m_ref[g] = top
            l_ref[g] = partial_sum(p)
            acc_ref[g] = weighted_t(n_full, p)

    def fixed_shift(j, carry):
        keys = keys_of(j)
        s = scores_t(keys, 0)
        for g in range(n_group):
            after = scores_t(keys, g + 1) if g + 1 < n_group else None
            p = jnp.exp2(s * scale - m_ref[g])
            l_ref[g] += partial_sum(p)
            acc_ref[g] += weighted_t(j, p)
            s = after
        return carry

    def running_max(j, carry):
        keys = keys_of(j)
        for g in range(n_group):
            s = scores_t(keys, g) * scale
            old = m_ref[g]
            top = jnp.maximum(old, jnp.max(s, axis=0, keepdims=True))
            alpha = jnp.exp2(old - top)
            p = jnp.exp2(s - top)
            m_ref[g] = top
            l_ref[g] = l_ref[g] * alpha + partial_sum(p)
            acc_ref[g] = acc_ref[g] * alpha + weighted_t(j, p)
        return carry

    diagonal()
    lax.fori_loop(0, n_full, fixed_shift, 0)

    largest = jnp.max(jnp.abs(acc_ref[...]).reshape(-1, lanes, n_tok), axis=0)
    sums = jnp.max(l_ref[...], axis=0)
    fine = jnp.where((largest < 1e36) & (sums < 1e30), 0.0, 1.0)

    @pl.when(jnp.max(fine) > 0.5)
    def _():
        diagonal()
        lax.fori_loop(0, n_full, running_max, 0)

    for g in range(n_group):
        out = acc_ref[g] / jnp.sum(l_ref[g], axis=0, keepdims=True)
        o_ref[0, :, g * HEAD_DIM:(g + 1) * HEAD_DIM] = out.T.astype(jnp.bfloat16)


def attention(qkv, kv, n_full, gathered):
    n_task, n_slot, n_tok, _ = qkv.shape
    n_group = n_slot - 2
    if gathered:
        n_piece = kv.shape[0]
        kv_spec = pl.BlockSpec((n_piece, 1, 2, n_tok, HEAD_DIM), lambda t, n: (0, t, 0, 0, 0))
    else:
        kv, n_piece = qkv, n_task
        kv_spec = pl.BlockSpec((n_piece, 2, n_tok, HEAD_DIM), lambda t, n: (0, n_group // 2, 0, 0))
    pairs = n_task * n_piece if gathered else n_task * (n_task + 1) // 2
    return pl.pallas_call(
        functools.partial(attention_kernel, gathered),
        grid_spec=pltpu.PrefetchScalarGridSpec(
            num_scalar_prefetch=1,
            grid=(n_task,),
            in_specs=[pl.BlockSpec((1, n_group, n_tok, HEAD_DIM), lambda t, n: (t, 0, 0, 0)), kv_spec],
            out_specs=pl.BlockSpec((1, n_tok, n_group * HEAD_DIM), lambda t, n: (t, 0, 0)),
            scratch_shapes=[
                pltpu.VMEM((n_group, HEAD_DIM, n_tok), jnp.bfloat16),
                pltpu.VMEM((n_piece, HEAD_DIM, n_tok), jnp.bfloat16),
                pltpu.VMEM((n_group, 1, n_tok), jnp.float32),
                pltpu.VMEM((n_group, 8, n_tok), jnp.float32),
                pltpu.VMEM((n_group, HEAD_DIM, n_tok), jnp.float32),
            ],
        ),
        out_shape=jax.ShapeDtypeStruct((n_task, n_tok, n_group * HEAD_DIM), jnp.bfloat16),
        compiler_params=pltpu.CompilerParams(vmem_limit_bytes=VMEM_LIMIT),
        cost_estimate=pl.CostEstimate(flops=2 * 4 * pairs * n_group * n_tok * n_tok * HEAD_DIM, bytes_accessed=16 << 20, transcendentals=0),
        name="attend",
    )(n_full, qkv, kv)


def out_kernel(x_ref, o_ref, w_ref, *refs):
    out_ref, flat_ref = refs[-2:]
    n_kv, _, cols = o_ref.shape

    @pl.when(pl.program_id(0) == 0)
    def _():
        for h in range(n_kv):
            flat_ref[:, h * cols:(h + 1) * cols] = o_ref[h]

    proj = jnp.dot(flat_ref[...], w_ref[...], preferred_element_type=jnp.float32)
    out_ref[0] = (x_ref[0].astype(jnp.float32) + proj).astype(jnp.bfloat16)


def out_project(prompt, tokens, heads, w_out, prev):
    n_batch, n_tok, d_model = tokens.shape
    n_kv, _, cols = heads.shape
    blk = 512
    in_specs = [
        pl.BlockSpec((1, n_tok, blk), lambda s: (prompt, 0, s)),
        pl.BlockSpec((n_kv, n_tok, cols), lambda s: (0, 0, 0)),
        pl.BlockSpec((n_kv * cols, blk), lambda s: (0, s)),
    ]
    args = [tokens, heads, w_out]
    aliases = {}
    if prev is not None:
        aliases = {3: 0}
        args.append(prev)
        in_specs.append(pl.BlockSpec(memory_space=pl.ANY))
    return pl.pallas_call(
        out_kernel,
        grid=(d_model // blk,),
        in_specs=in_specs,
        out_specs=pl.BlockSpec((1, n_tok, blk), lambda s: (prompt, 0, s)),
        out_shape=jax.ShapeDtypeStruct((n_batch, n_tok, d_model), jnp.bfloat16),
        scratch_shapes=[pltpu.VMEM((n_tok, n_kv * cols), jnp.bfloat16)],
        input_output_aliases=aliases,
        compiler_params=pltpu.CompilerParams(vmem_limit_bytes=VMEM_LIMIT),
        cost_estimate=pl.CostEstimate(flops=2 * n_tok * n_kv * cols * d_model, bytes_accessed=32 << 20, transcendentals=0),
        name="outproj",
    )(*args)


def solution(mesh):
    def per_device(tokens, w_query, w_key, w_value, w_out, attn_norm, q_norm, k_norm):
        n_batch, seq_loc, _ = tokens.shape
        n_kv = w_key.shape[1] // HEAD_DIM
        me = lax.axis_index('sp')
        cos_t, sin_t = rope_tables(me * seq_loc + jnp.arange(seq_loc))
        norms = (attn_norm.reshape(1, -1), q_norm.reshape(1, -1), k_norm.reshape(1, -1))
        n_full = me.astype(jnp.int32).reshape(1)
        caches, out, last = None, None, None
        sent, mixed = {}, {}

        def after_last(value):
            return value if last is None else lax.optimization_barrier((value, last))[0]

        def exchange(value):
            return lax.all_to_all(value, 'sp', 0, 0, tiled=True)

        for kind, b in ORDER:
            split = b < N_SPLIT
            if kind == 'qkv':
                send, kc, vc = qkv_project(b, after_last(tokens), w_query, w_key, w_value, *norms, cos_t, sin_t, caches)
                caches = (kc, vc)
                if split:
                    sent[b] = (exchange(send), None)
                else:
                    sent[b] = (send, lax.all_gather(send[:, -2:], 'sp'))
                last = send
            elif kind == 'att':
                o = attention(after_last(sent[b][0]), sent[b][1], n_full, not split)
                mixed[b] = exchange(o) if split else o
                last = o
            else:
                out = out_project(b, tokens, after_last(mixed[b]), w_out, out)
                last = out
        cache_shape = (n_batch, seq_loc, n_kv, HEAD_DIM)
        return out, caches[0].reshape(cache_shape), caches[1].reshape(cache_shape)

    spec_tok = P('dp', 'sp', None)
    spec_cache = P('dp', 'sp', None, None)
    spec_mat = P(None, None)
    spec_vec = P(None)

    return jax.shard_map(per_device, mesh=mesh, in_specs=(spec_tok, spec_mat, spec_mat, spec_mat, spec_mat, spec_vec, spec_vec, spec_vec), out_specs=(spec_tok, spec_cache, spec_cache), check_vma=False)
```
